128 devices in a mesh: kv: 64 (over z, x, y), head: 2 (over core).
Axes of the slice: x: 4, y: 4, z: 4, core: 2. Of those that a mesh axis runs over, the one named last changes fastest.
Arguments:
- queries: bfloat16 [8, 256, 128], P('head', 'kv'), may hold values from -384 to 384
- key_cache: bfloat16 [4096, 8, 128, 128], P('kv', 'head'), may hold values from -6 to 6
- value_cache: bfloat16 [4096, 8, 128, 128], P('kv', 'head'), may hold values from -6 to 6
- key_new: bfloat16 [32, 8, 128], P(None, 'head'), may hold values from -6 to 6
- value_new: bfloat16 [32, 8, 128], P(None, 'head'), may hold values from -6 to 6
- lengths: int32 [32], replicated, may hold values from 2 to 16385, as said below
- page_table: int32 [4096], replicated, may hold values from 0 to 4095, each once
Outputs:
- attended: bfloat16 [8, 256, 128], P('head', 'kv')
The draws below stay inside these ranges and needn't reach their ends.
Inputs may be any that keep to these rules, and one draw needn't show every extreme that they name: The cache holds the first lengths[s] - 1 tokens of sequence s; some sequence has the largest length. `page_table`: every page appears once; page g lies on kv index g // 64.
All inputs are finite; a program needn't handle non-finite values.
Results may differ from the reference program's by a relative error of at most 0.0025.
Values may be sent and summed in bfloat16 or wider, within the bound.
A program may use at most 64 MiB of HBM per device.

```python
import math
import jax
import jax.numpy as jnp
from jax import lax

QH = 64
KVH = 8
HD = 128
PAGE = 128
MAXP = 128
SEQS = 32
PAGES = 4096


def draw_queries(key, part):
    normal_part = jax.random.normal(jax.random.fold_in(key, 11), (KVH, SEQS * (QH // KVH), HD), jnp.float32)
    values = jnp.clip(normal_part * 2.0, -8.0, 8.0)
    return values.astype(jnp.bfloat16)


def draw_lengths(key, part):
    most = MAXP * PAGE + 1
    values = jax.random.randint(jax.random.fold_in(key, 21), (SEQS,), 2, most + 1, jnp.int32)
    chosen = jax.random.randint(jax.random.fold_in(key, 22), (), 0, SEQS, jnp.int32)
    return jnp.where(jnp.arange(SEQS, dtype=jnp.int32) == chosen, most, values).astype(jnp.int32)


def block_levels(rng, shape, shards, low, largest):
    level, own = 1.0, jax.random.fold_in(rng, 6)
    for axis_at, shards_of in shards:
        draws = jnp.exp(jax.random.uniform(jax.random.fold_in(own, axis_at), (shards_of,), jnp.float32, low / len(shards), largest / len(shards)))
        level = level * jnp.repeat(draws, shape[axis_at] // shards_of).reshape([-1 if axis == axis_at else 1 for axis in range(len(shape))])
    return level


def noise(rng, dims, width, most, pieces=(), held_as=jnp.bfloat16):
    gain = block_levels(rng, dims, pieces, -0.22, 0.18) if pieces else 1.0
    entries = jax.random.normal(rng, dims, jnp.float32) * width * gain
    return jnp.minimum(jnp.maximum(entries, -most), most).astype(held_as)


def setup_inputs(seed: int = 0) -> dict:
    key_of = jax.random.split(jax.random.key(seed), 8)
    queries = draw_queries(jax.random.fold_in(key_of[7], 71), 0)
    key_cache = noise(key_of[1], (PAGES, KVH, PAGE, HD), 1.0, 6.0, ((0, 64), (1, 2)))
    value_cache = noise(key_of[2], (PAGES, KVH, PAGE, HD), 1.0, 6.0, ((0, 64), (1, 2)))
    key_new = noise(key_of[3], (SEQS, KVH, HD), 1.0, 6.0, ((1, 2),))
    value_new = noise(key_of[4], (SEQS, KVH, HD), 1.0, 6.0, ((1, 2),))
    lengths = draw_lengths(jax.random.fold_in(key_of[7], 71), 0)
    page_table = jax.random.permutation(key_of[6], PAGES).astype(jnp.int32)
    return {"queries": queries, "key_cache": key_cache, "value_cache": value_cache, "key_new": key_new, "value_new": value_new, "lengths": lengths, "page_table": page_table}


LOWEST_SCORE = -1e+30

def finish(cache_max, cache_sum, cache_out, query_wide, fresh_key, fresh_value, score_scale):
    new_score = lax.optimization_barrier(jnp.sum(query_wide * fresh_key.astype(jnp.float32), axis=-1)) * score_scale
    highest = jnp.maximum(cache_max, new_score)
    old_part = jnp.exp(cache_max - highest)
    new_part = jnp.exp(new_score - highest)
    numerator = cache_out * old_part[..., None] + new_part[..., None] * fresh_value.astype(jnp.float32)
    denominator = cache_sum * old_part + new_part
    return (numerator / denominator[..., None]).astype(jnp.bfloat16)

def reference(queries, key_cache, value_cache, key_new, value_new, lengths, page_table):
    seq_count = lengths.shape[0]
    kv_count = queries.shape[0]
    head_width = queries.shape[2]
    group_size = queries.shape[1] // seq_count
    page_total = key_cache.shape[0]
    page_len = key_cache.shape[2]
    page_slots = page_total // seq_count
    score_scale = 1.0 / math.sqrt(head_width)
    table = page_table.reshape(seq_count, page_slots).astype(jnp.int32)
    grouped = jnp.transpose(queries.reshape(kv_count, seq_count, group_size, head_width), (1, 0, 2, 3))
    offsets = jnp.arange(page_slots, dtype=jnp.int32)[:, None] * page_len + jnp.arange(page_len, dtype=jnp.int32)[None, :]

    def one_sequence(packed):
        query_rows, page_ids, length, fresh_key, fresh_value = packed
        keys = key_cache[page_ids].astype(jnp.float32)
        values = value_cache[page_ids].astype(jnp.float32)
        query_wide = query_rows.astype(jnp.float32)
        scores = jnp.einsum('gqd,mgtd->mgqt', query_wide, keys, precision=lax.Precision.HIGHEST) * score_scale
        in_cache = (offsets < length - 1)[:, None, None, :]
        masked = jnp.where(in_cache, scores, LOWEST_SCORE)
        page_max = lax.optimization_barrier(jnp.max(masked, axis=3))
        weights = jnp.where(in_cache, jnp.exp(masked - page_max[..., None]), 0.0)
        page_sum = lax.optimization_barrier(jnp.sum(weights, axis=3))
        rounded = lax.optimization_barrier(weights.astype(jnp.bfloat16)).astype(jnp.float32)
        page_out = jnp.einsum('mgqt,mgtd->mgqd', rounded, values, precision=lax.Precision.HIGHEST)
        cache_max = lax.optimization_barrier(jnp.max(page_max, axis=0))
        factor = jnp.exp(page_max - cache_max[None])
        cache_sum = lax.optimization_barrier(jnp.sum(page_sum * factor, axis=0))
        cache_out = lax.optimization_barrier(jnp.sum(page_out * factor[..., None], axis=0))
        return finish(cache_max, cache_sum, cache_out, query_wide, fresh_key[:, None, :], fresh_value[:, None, :], score_scale)
    result = lax.map(one_sequence, (grouped, table, lengths.astype(jnp.int32), key_new, value_new))
    return jnp.transpose(result, (1, 0, 2, 3)).reshape(kv_count, seq_count * group_size, head_width)
```

```python
import functools
import math

import jax
import jax.numpy as jnp
from jax import lax
from jax.experimental import pallas as pl
from jax.experimental.pallas import tpu as pltpu
from jax.sharding import PartitionSpec as P

LOW = -1e30
FLOOR = -5e29
F32 = jnp.float32
BF16 = jnp.bfloat16


def hops(t):
    total = 0
    while t:
        total += (0, 1, 2, 1)[t % 4]
        t //= 4
    return total


def iota(shape, dim):
    return lax.broadcasted_iota(jnp.int32, shape, dim)


def dot(a, b, dims=((1,), (0,))):
    return lax.dot_general(a, b, (dims, ((), ())), preferred_element_type=F32)


def kernel(
    n, q_ref, k_hbm, v_hbm, kn_ref, vn_ref, len_ref, tbl_ref, out_ref,
    kbuf, vbuf, qall, racc, rml, sbuf, sacc, sstat, gacc, gstat, meta_v, meta_s,
    ksem, vsem, msem, qs_sem, qr_sem, as_sem, ar_sem, ss_sem, sr_sem,
):
    pages, heads, page_len, width = kbuf.shape
    seqs = len_ref.shape[0]
    slots = tbl_ref.shape[1]
    me = lax.axis_index("kv")
    head = lax.axis_index("head")
    c = math.log2(math.e) / math.sqrt(width)
    order = sorted(range(1, n), key=hops, reverse=True)

    def peer(t):
        return (jnp.bitwise_xor(me, t), head)

    parts = 8
    step = pages // parts
    for hbm, buf, sem in ((k_hbm, kbuf, ksem), (v_hbm, vbuf, vsem)):
        for i in range(parts):
            pltpu.make_async_copy(hbm.at[pl.ds(i * step, step)], buf.at[pl.ds(i * step, step)], sem).start()

    barrier = pltpu.get_barrier_semaphore()
    for t in order:
        pl.semaphore_signal(barrier, inc=1, device_id=peer(t), device_id_type=pl.DeviceIdType.MESH)

    q16 = q_ref[...].astype(F32).reshape(16, width)
    qall[me] = q16.astype(BF16)

    pl.semaphore_wait(barrier, n - 1)
    for t in order:
        pltpu.make_async_remote_copy(
            src_ref=qall.at[me], dst_ref=qall.at[me], send_sem=qs_sem, recv_sem=qr_sem,
            device_id=peer(t), device_id_type=pl.DeviceIdType.MESH,
        ).start()

    rel = tbl_ref[...] - me * pages
    here = jnp.logical_and(rel >= 0, rel < pages)
    here_f = jnp.where(here, 1.0, 0.0)
    here_b = here_f.astype(BF16)
    upper = jnp.where(iota((slots, slots), 0) < iota((slots, slots), 1), 1.0, 0.0).astype(BF16)
    ones = jnp.full((slots, slots), 1.0, BF16)
    lower = jnp.where(iota((seqs, seqs), 1) < iota((seqs, seqs), 0), 1.0, 0.0).astype(BF16)
    in_row = dot(here_b, upper)
    row_total = dot(here_b, ones)
    before = dot(lower, row_total.astype(BF16))
    place = jnp.where(here, in_row + before, -1.0)
    value = ((iota((seqs, slots), 0) * slots + iota((seqs, slots), 1)) * pages + rel).astype(F32)
    value = jnp.where(here, value, 0.0)
    kth = iota((pages, slots), 0).astype(F32)
    found = jnp.zeros((pages, slots), F32)
    for s in range(seqs):
        found = found + jnp.where(place[s : s + 1] == kth, value[s : s + 1], 0.0)
    found = jnp.sum(found, axis=1, keepdims=True)
    lane = iota((pages, slots), 1)
    row = jnp.sum(jnp.where(lane == iota((pages, slots), 0), found, 0.0), axis=0, keepdims=True)
    ends = before + row_total
    lane = iota((seqs, slots), 1)
    row = row + jnp.sum(jnp.where(lane == iota((seqs, slots), 0) + pages, ends, 0.0), axis=0, keepdims=True)
    meta_v[...] = row.astype(jnp.int32)
    copy = pltpu.make_async_copy(meta_v, meta_s, msem)
    copy.start()

    owned = me // 2
    row_g = iota((16, width), 0) // 4
    kn = kn_ref[owned].astype(F32)
    vn = vn_ref[owned].astype(F32)
    kn16 = jnp.zeros((16, width), F32)
    vn16 = jnp.zeros((16, width), F32)
    for g in range(heads):
        kn16 = jnp.where(row_g == g, kn[g : g + 1], kn16)
        vn16 = jnp.where(row_g == g, vn[g : g + 1], vn16)
    new_raw = jnp.sum(q16 * kn16, axis=1, keepdims=True)

    copy.wait()
    pltpu.make_async_copy(k_hbm, kbuf, ksem).wait()
    pltpu.make_async_copy(v_hbm, vbuf, vsem).wait()
    pltpu.make_async_copy(qall.at[pl.ds(0, n - 1)], qall.at[pl.ds(0, n - 1)], qr_sem).wait()

    low_half = iota((8, page_len), 0) < 4
    low_half16 = iota((16, page_len), 0) % 8 < 4
    lanes = iota((32, page_len), 1)
    chunk = sbuf.shape[0]
    page_bits = pages.bit_length() - 1
    slot_bits = slots.bit_length() - 1

    def decode(k):
        code = meta_s[0, k]
        slot = jnp.bitwise_and(code >> page_bits, slots - 1)
        seq = jnp.bitwise_and(code >> (page_bits + slot_bits), seqs - 1)
        return jnp.bitwise_and(code, pages - 1), seq, slot

    def scores(k):
        p, s, _ = decode(k)
        qb = qall[pl.ds(2 * s, 2)].reshape(32, width)
        raw = dot(qb, kbuf[p].reshape(heads * page_len, width), ((1,), (1,)))
        tiles = []
        for rb in range(4):
            g = 2 * (rb % 2)
            mine = raw[rb * 8 : rb * 8 + 8]
            tiles.append(jnp.where(low_half, mine[:, g * 128 : g * 128 + 128], mine[:, g * 128 + 128 : g * 128 + 256]))
        return jnp.concatenate(tiles, axis=0)

    def attend(k, raw, state):
        m, l, acc = state
        p, s, slot = decode(k)
        before_seq = decode(jnp.maximum(k - 1, 0))[1]
        first = jnp.logical_or(k == 0, before_seq != s)
        valid = len_ref[s] - 1 - slot * page_len
        raw = jnp.where(lanes < valid, raw, LOW)
        top = jnp.maximum(jnp.max(raw, axis=1, keepdims=True), FLOOR)
        weights = jnp.exp2((raw - top) * c)
        total = jnp.sum(weights, axis=1, keepdims=True)
        outs = []
        for pair in range(2):
            both = jnp.concatenate(
                [weights[pair * 8 : pair * 8 + 8], weights[16 + pair * 8 : 16 + pair * 8 + 8]], axis=0
            )
            lhs = jnp.concatenate(
                [jnp.where(low_half16, both, 0.0).astype(BF16), jnp.where(low_half16, 0.0, both).astype(BF16)], axis=1
            )
            rhs = vbuf[p, pl.ds(2 * pair, 2)].reshape(2 * page_len, width)
            outs.append(dot(lhs, rhs))
        page_out = jnp.concatenate([outs[0][:8], outs[1][:8], outs[0][8:], outs[1][8:]], axis=0)
        top = jnp.broadcast_to(top, m.shape)
        m = jnp.where(first, FLOOR, m)
        new_m = jnp.maximum(m, top)
        old = jnp.where(first, 0.0, jnp.exp2((m - new_m) * c))
        new = jnp.exp2((top - new_m) * c)
        l = l * old + total * new
        acc = acc * old + page_out * new
        racc[k] = acc
        rml[k] = jnp.where(lanes < 64, new_m, l)
        return new_m, l, acc

    for i in range(chunk):
        sbuf[i] = scores(i)

    def body(i, state):
        raws = [sbuf[u] for u in range(chunk)]
        for u in range(chunk):
            sbuf[u] = scores((i + 1) * chunk + u)
        for u in range(chunk):
            state = attend(i * chunk + u, raws[u], state)
        return state

    zero = jnp.zeros((32, width), F32)
    steps = pages // chunk
    state = lax.fori_loop(0, steps - 1, body, (zero, zero, zero))
    for u in range(chunk):
        state = attend((steps - 1) * chunk + u, sbuf[u], state)

    lane16 = iota((16, width), 1) % 64

    def gather(s, stat):
        end = meta_s[0, pages + s]
        start = jnp.where(s == 0, 0, meta_s[0, pages + jnp.maximum(s - 1, 0)])
        some = end > start
        last = jnp.clip(end - 1, 0, pages - 1)
        acc = jnp.where(some, racc[last], 0.0)
        ml = jnp.where(some, rml[last], jnp.where(lanes < 64, FLOOR, 0.0))
        sacc[2 * s] = acc[:16]
        sacc[2 * s + 1] = acc[16:]
        stat = jnp.where(lane16 == 2 * s, ml[:16], stat)
        return jnp.where(lane16 == 2 * s + 1, ml[16:], stat)

    stat = lax.fori_loop(0, seqs, gather, jnp.zeros((16, width), F32), unroll=4)
    for t in order:
        to = jnp.bitwise_xor(me, t)
        pltpu.make_async_remote_copy(
            src_ref=sacc.at[to], dst_ref=gacc.at[me], send_sem=as_sem, recv_sem=ar_sem,
            device_id=peer(t), device_id_type=pl.DeviceIdType.MESH,
        ).start()
    turned = jnp.concatenate([stat] * 8, axis=0).T
    sstat[:, 0, :] = turned[:n]
    sstat[:, 1, :] = turned[n:]
    for t in order:
        to = jnp.bitwise_xor(me, t)
        pltpu.make_async_remote_copy(
            src_ref=sstat.at[to], dst_ref=gstat.at[me], send_sem=ss_sem, recv_sem=sr_sem,
            device_id=peer(t), device_id_type=pl.DeviceIdType.MESH,
        ).start()
    gacc[me] = sacc[me]
    gstat[me] = sstat[me]

    some_q, some_a, some_s = (r.at[pl.ds(0, n - 1)] for r in (qall, gacc, gstat))
    pltpu.make_async_copy(some_s, some_s, sr_sem).wait()
    tops = gstat[:, 0, :]
    sums = gstat[:, 1, :]
    top = jnp.max(tops, axis=0, keepdims=True)
    w = jnp.exp2((tops - top) * c)
    total = jnp.sum(w * sums, axis=0, keepdims=True)
    at_row = iota((16, width), 1) % 16 == iota((16, width), 0)
    first16 = jnp.logical_and(at_row, iota((16, width), 1) < 16)
    top16 = jnp.sum(jnp.where(first16, top, 0.0), axis=1, keepdims=True)
    sum16 = jnp.sum(jnp.where(first16, total, 0.0), axis=1, keepdims=True)
    mine = iota((8, width), 1) // 16 == iota((8, width), 0)
    blocks = []
    for b in range(n // 8):
        line = jnp.sum(jnp.where(mine, w[8 * b : 8 * b + 8], 0.0), axis=0, keepdims=True)
        blocks.append(jnp.where(at_row, line, 0.0))
    wide = jnp.concatenate(blocks, axis=1)
    wide_hi = wide.astype(BF16)
    wide_lo = (wide - wide_hi.astype(F32)).astype(BF16)
    high = jnp.maximum(top16, new_raw)
    old = jnp.exp2((top16 - high) * c)
    new = jnp.exp2((new_raw - high) * c)
    pltpu.make_async_copy(some_a, some_a, ar_sem).wait()
    sent = gacc[...].reshape(16 * n, width)
    sent_hi = sent.astype(BF16)
    sent_lo = (sent - sent_hi.astype(F32)).astype(BF16)
    both = dot(jnp.concatenate([wide_hi, wide_lo], axis=0), sent_hi)
    numer = (both[:16] + both[16:] + dot(wide_hi, sent_lo)) * old + new * vn16
    out_ref[...] = (numer / (sum16 * old + new)).astype(BF16)

    pltpu.make_async_copy(some_q, some_q, qs_sem).wait()
    pltpu.make_async_copy(some_a, some_a, as_sem).wait()
    pltpu.make_async_copy(some_s, some_s, ss_sem).wait()


def on_device(queries, key_cache, value_cache, key_new, value_new, lengths, page_table):
    n = lax.axis_size("kv")
    heads, rows, width = queries.shape
    pages, _, page_len, _ = key_cache.shape
    seqs = lengths.shape[0]
    vmem = pl.BlockSpec(memory_space=pltpu.VMEM)
    hbm = pl.BlockSpec(memory_space=pltpu.HBM)
    dma = pltpu.SemaphoreType.DMA
    out = pl.pallas_call(
        functools.partial(kernel, n),
        out_shape=jax.ShapeDtypeStruct((heads * rows, width), BF16),
        in_specs=[vmem, hbm, hbm, vmem, vmem, pl.BlockSpec(memory_space=pltpu.SMEM), vmem],
        out_specs=vmem,
        scratch_shapes=[
            pltpu.VMEM(key_cache.shape, BF16),
            pltpu.VMEM(value_cache.shape, BF16),
            pltpu.VMEM((n, 16, width), BF16),
            pltpu.VMEM((pages, 32, width), F32),
            pltpu.VMEM((pages, 32, width), F32),
            pltpu.VMEM((4, 32, page_len), F32),
            pltpu.VMEM((n, 16, width), F32),
            pltpu.VMEM((n, 2, width), F32),
            pltpu.VMEM((n, 16, width), F32),
            pltpu.VMEM((n, 2, width), F32),
            pltpu.VMEM((1, width), jnp.int32),
            pltpu.SMEM((1, width), jnp.int32),
            *[dma] * 9,
        ],
        compiler_params=pltpu.CompilerParams(
            collective_id=0, has_side_effects=True
        ),
    )(queries, key_cache, value_cache, key_new, value_new, lengths, page_table.reshape(seqs, -1))
    return out.reshape(heads, rows, width)


def solution(mesh):
    placed = (
        P("head", "kv", None),
        P("kv", "head", None, None),
        P("kv", "head", None, None),
        P(None, "head", None),
        P(None, "head", None),
        P(),
        P(),
    )
    return jax.shard_map(
        on_device, mesh=mesh, in_specs=placed, out_specs=P("head", "kv", None), check_vma=False
    )
```

```python
import functools
import math

import jax
import jax.numpy as jnp
from jax import lax
from jax.experimental import pallas as pl
from jax.experimental.pallas import tpu as pltpu
from jax.sharding import PartitionSpec as P

LOW = -1e30
FLOOR = -5e29
F32 = jnp.float32
BF16 = jnp.bfloat16


def hops(t):
    total = 0
    while t:
        total += (0, 1, 2, 1)[t % 4]
        t //= 4
    return total


def iota(shape, dim):
    return lax.broadcasted_iota(jnp.int32, shape, dim)


def dot(a, b, dims=((1,), (0,))):
    return lax.dot_general(a, b, (dims, ((), ())), preferred_element_type=F32)


def kernel(
    n, q_hbm, k_hbm, v_hbm, kn_hbm, vn_hbm, len_hbm, tbl_hbm, out_ref,
    q_ref, kn_ref, vn_ref, len_ref, tbl_ref,
    kbuf, vbuf, qall, racc, rml, sbuf, sacc, sstat, gacc, gstat, meta_v, meta_s,
    ksem, vsem, qsem, insem, lsem, msem, qs_sem, qr_sem, as_sem, ar_sem, ss_sem, sr_sem,
):
    pages, heads, page_len, width = kbuf.shape
    seqs = len_ref.shape[0]
    slots = tbl_ref.shape[1]
    me = lax.axis_index("kv")
    head = lax.axis_index("head")
    c = math.log2(math.e) / math.sqrt(width)
    order = sorted(range(1, n), key=hops, reverse=True)

    def peer(t):
        return (jnp.bitwise_xor(me, t), head)

    barrier = pltpu.get_barrier_semaphore()
    for t in order:
        pl.semaphore_signal(barrier, inc=1, device_id=peer(t), device_id_type=pl.DeviceIdType.MESH)

    owned = me // 2
    q_copy = pltpu.make_async_copy(q_hbm, q_ref, qsem)
    q_copy.start()
    len_copy = pltpu.make_async_copy(len_hbm, len_ref, lsem)
    len_copy.start()
    small = [
        pltpu.make_async_copy(tbl_hbm, tbl_ref, insem.at[0]),
        pltpu.make_async_copy(kn_hbm.at[owned], kn_ref, insem.at[1]),
        pltpu.make_async_copy(vn_hbm.at[owned], vn_ref, insem.at[2]),
    ]
    for one in small:
        one.start()
    q_copy.wait()
    len_copy.wait()
    for one in small:
        one.wait()
    parts = 8
    step = pages // parts
    for hbm, buf, sem in ((k_hbm, kbuf, ksem), (v_hbm, vbuf, vsem)):
        for i in range(parts):
            pltpu.make_async_copy(hbm.at[pl.ds(i * step, step)], buf.at[pl.ds(i * step, step)], sem).start()

    q16 = q_ref[...].astype(F32).reshape(16, width)
    qall[me] = q16.astype(BF16)


    rel = tbl_ref[...] - me * pages
    here = jnp.logical_and(rel >= 0, rel < pages)
    here_f = jnp.where(here, 1.0, 0.0)
    here_b = here_f.astype(BF16)
    upper = jnp.where(iota((slots, slots), 0) < iota((slots, slots), 1), 1.0, 0.0).astype(BF16)
    ones = jnp.full((slots, slots), 1.0, BF16)
    lower = jnp.where(iota((seqs, seqs), 1) < iota((seqs, seqs), 0), 1.0, 0.0).astype(BF16)
    in_row = dot(here_b, upper)
    row_total = dot(here_b, ones)
    before = dot(lower, row_total.astype(BF16))
    place = jnp.where(here, in_row + before, -1.0)
    value = ((iota((seqs, slots), 0) * slots + iota((seqs, slots), 1)) * pages + rel).astype(F32)
    value = jnp.where(here, value, 0.0)
    kth = iota((pages, slots), 0).astype(F32)
    found = jnp.zeros((pages, slots), F32)
    for s in range(seqs):
        found = found + jnp.where(place[s : s + 1] == kth, value[s : s + 1], 0.0)
    found = jnp.sum(found, axis=1, keepdims=True)
    lane = iota((pages, slots), 1)
    row = jnp.sum(jnp.where(lane == iota((pages, slots), 0), found, 0.0), axis=0, keepdims=True)
    ends = before + row_total
    lane = iota((seqs, slots), 1)
    row = row + jnp.sum(jnp.where(lane == iota((seqs, slots), 0) + pages, ends, 0.0), axis=0, keepdims=True)
    meta_v[...] = row.astype(jnp.int32)
    copy = pltpu.make_async_copy(meta_v, meta_s, msem)
    copy.start()

    row_g = iota((16, width), 0) // 4
    kn = kn_ref[...].astype(F32)
    vn = vn_ref[...].astype(F32)
    kn16 = jnp.zeros((16, width), F32)
    vn16 = jnp.zeros((16, width), F32)
    for g in range(heads):
        kn16 = jnp.where(row_g == g, kn[g : g + 1], kn16)
        vn16 = jnp.where(row_g == g, vn[g : g + 1], vn16)
    new_raw = jnp.sum(q16 * kn16, axis=1, keepdims=True)

    copy.wait()

    pl.semaphore_wait(barrier, n - 1)
    for t in order:
        pltpu.make_async_remote_copy(
            src_ref=qall.at[me], dst_ref=qall.at[me], send_sem=qs_sem, recv_sem=qr_sem,
            device_id=peer(t), device_id_type=pl.DeviceIdType.MESH,
        ).start()

    pltpu.make_async_copy(k_hbm, kbuf, ksem).wait()
    pltpu.make_async_copy(v_hbm, vbuf, vsem).wait()
    pltpu.make_async_copy(qall.at[pl.ds(0, n - 1)], qall.at[pl.ds(0, n - 1)], qr_sem).wait()

    even = (iota((32, width), 0) // 4) % 2 == 0
    low_half16 = iota((16, page_len), 0) % 8 < 4
    lanes = iota((32, page_len), 1)
    chunk = sbuf.shape[0]
    page_bits = pages.bit_length() - 1
    slot_bits = slots.bit_length() - 1

    def decode(k):
        code = meta_s[0, k]
        slot = jnp.bitwise_and(code >> page_bits, slots - 1)
        seq = jnp.bitwise_and(code >> (page_bits + slot_bits), seqs - 1)
        return jnp.bitwise_and(code, pages - 1), seq, slot

    def scores(k):
        p, s, _ = decode(k)
        qb = qall[pl.ds(2 * s, 2)].reshape(32, width)
        none = jnp.zeros_like(qb)
        lhs = jnp.concatenate([jnp.where(even, qb, none), jnp.where(even, none, qb)], axis=1)
        keys = kbuf[p]
        rhs = jnp.concatenate(
            [jnp.concatenate([keys[0], keys[1]], axis=1), jnp.concatenate([keys[2], keys[3]], axis=1)], axis=0
        )
        raw = dot(lhs, rhs, ((1,), (1,)))
        return jnp.concatenate(
            [raw[0:8, :page_len], raw[8:16, page_len:], raw[16:24, :page_len], raw[24:32, page_len:]], axis=0
        )

    def attend(k, raw, state):
        m, l, acc = state
        p, s, slot = decode(k)
        before_seq = decode(jnp.maximum(k - 1, 0))[1]
        first = jnp.logical_or(k == 0, before_seq != s)
        valid = len_ref[s] - 1 - slot * page_len
        raw = jnp.where(lanes < valid, raw, LOW)
        top = jnp.maximum(jnp.max(raw, axis=1, keepdims=True), FLOOR)
        weights = jnp.exp2((raw - top) * c)
        total = jnp.sum(weights, axis=1, keepdims=True)
        outs = []
        for pair in range(2):
            both = jnp.concatenate(
                [weights[pair * 8 : pair * 8 + 8], weights[16 + pair * 8 : 16 + pair * 8 + 8]], axis=0
            )
            lhs = jnp.concatenate(
                [jnp.where(low_half16, both, 0.0).astype(BF16), jnp.where(low_half16, 0.0, both).astype(BF16)], axis=1
            )
            rhs = vbuf[p, pl.ds(2 * pair, 2)].reshape(2 * page_len, width)
            outs.append(dot(lhs, rhs))
        page_out = jnp.concatenate([outs[0][:8], outs[1][:8], outs[0][8:], outs[1][8:]], axis=0)
        top = jnp.broadcast_to(top, m.shape)
        m = jnp.where(first, FLOOR, m)
        new_m = jnp.maximum(m, top)
        old = jnp.where(first, 0.0, jnp.exp2((m - new_m) * c))
        new = jnp.exp2((top - new_m) * c)
        l = l * old + total * new
        acc = acc * old + page_out * new
        racc[k] = acc
        rml[k] = jnp.where(lanes < 64, new_m, l)
        return new_m, l, acc

    for i in range(chunk):
        sbuf[i] = scores(i)

    def body(i, state):
        raws = [sbuf[u] for u in range(chunk)]
        for u in range(chunk):
            sbuf[u] = scores((i + 1) * chunk + u)
        for u in range(chunk):
            state = attend(i * chunk + u, raws[u], state)
        return state

    zero = jnp.zeros((32, width), F32)
    steps = pages // chunk
    state = lax.fori_loop(0, steps - 1, body, (zero, zero, zero))
    for u in range(chunk):
        state = attend((steps - 1) * chunk + u, sbuf[u], state)

    lane16 = iota((16, width), 1) % 64

    def gather(s, stat):
        end = meta_s[0, pages + s]
        start = jnp.where(s == 0, 0, meta_s[0, pages + jnp.maximum(s - 1, 0)])
        some = end > start
        last = jnp.clip(end - 1, 0, pages - 1)
        acc = jnp.where(some, racc[last], 0.0)
        ml = jnp.where(some, rml[last], jnp.where(lanes < 64, FLOOR, 0.0))
        sacc[2 * s] = acc[:16]
        sacc[2 * s + 1] = acc[16:]
        stat = jnp.where(lane16 == 2 * s, ml[:16], stat)
        return jnp.where(lane16 == 2 * s + 1, ml[16:], stat)

    stat = lax.fori_loop(0, seqs, gather, jnp.zeros((16, width), F32), unroll=4)
    for t in order:
        to = jnp.bitwise_xor(me, t)
        pltpu.make_async_remote_copy(
            src_ref=sacc.at[to], dst_ref=gacc.at[me], send_sem=as_sem, recv_sem=ar_sem,
            device_id=peer(t), device_id_type=pl.DeviceIdType.MESH,
        ).start()
    turned = jnp.concatenate([stat] * 8, axis=0).T
    sstat[:, 0, :] = turned[:n]
    sstat[:, 1, :] = turned[n:]
    for t in order:
        to = jnp.bitwise_xor(me, t)
        pltpu.make_async_remote_copy(
            src_ref=sstat.at[to], dst_ref=gstat.at[me], send_sem=ss_sem, recv_sem=sr_sem,
            device_id=peer(t), device_id_type=pl.DeviceIdType.MESH,
        ).start()
    gacc[me] = sacc[me]
    gstat[me] = sstat[me]

    some_q, some_a, some_s = (r.at[pl.ds(0, n - 1)] for r in (qall, gacc, gstat))
    pltpu.make_async_copy(some_s, some_s, sr_sem).wait()
    tops = gstat[:, 0, :]
    sums = gstat[:, 1, :]
    top = jnp.max(tops, axis=0, keepdims=True)
    w = jnp.exp2((tops - top) * c)
    total = jnp.sum(w * sums, axis=0, keepdims=True)
    at_row = iota((16, width), 1) % 16 == iota((16, width), 0)
    first16 = jnp.logical_and(at_row, iota((16, width), 1) < 16)
    top16 = jnp.sum(jnp.where(first16, top, 0.0), axis=1, keepdims=True)
    sum16 = jnp.sum(jnp.where(first16, total, 0.0), axis=1, keepdims=True)
    mine = iota((8, width), 1) // 16 == iota((8, width), 0)
    blocks = []
    for b in range(n // 8):
        line = jnp.sum(jnp.where(mine, w[8 * b : 8 * b + 8], 0.0), axis=0, keepdims=True)
        blocks.append(jnp.where(at_row, line, 0.0))
    wide = jnp.concatenate(blocks, axis=1)
    wide_hi = wide.astype(BF16)
    wide_lo = (wide - wide_hi.astype(F32)).astype(BF16)
    high = jnp.maximum(top16, new_raw)
    old = jnp.exp2((top16 - high) * c)
    new = jnp.exp2((new_raw - high) * c)
    pltpu.make_async_copy(some_a, some_a, ar_sem).wait()
    sent = gacc[...].reshape(16 * n, width)
    sent_hi = sent.astype(BF16)
    sent_lo = (sent - sent_hi.astype(F32)).astype(BF16)
    both = dot(jnp.concatenate([wide_hi, wide_lo], axis=0), sent_hi)
    numer = (both[:16] + both[16:] + dot(wide_hi, sent_lo)) * old + new * vn16
    out_ref[...] = (numer / (sum16 * old + new)).reshape(out_ref.shape).astype(BF16)

    pltpu.make_async_copy(some_q, some_q, qs_sem).wait()
    pltpu.make_async_copy(some_a, some_a, as_sem).wait()
    pltpu.make_async_copy(some_s, some_s, ss_sem).wait()


def on_device(queries, key_cache, value_cache, key_new, value_new, lengths, page_table):
    n = lax.axis_size("kv")
    heads, rows, width = queries.shape
    pages, _, page_len, _ = key_cache.shape
    seqs = lengths.shape[0]
    vmem = pl.BlockSpec(memory_space=pltpu.VMEM)
    hbm = pl.BlockSpec(memory_space=pltpu.HBM)
    dma = pltpu.SemaphoreType.DMA
    out = pl.pallas_call(
        functools.partial(kernel, n),
        out_shape=jax.ShapeDtypeStruct(queries.shape, BF16),
        in_specs=[hbm] * 7,
        out_specs=vmem,
        scratch_shapes=[
            pltpu.VMEM(queries.shape, BF16),
            pltpu.VMEM((heads, width), BF16),
            pltpu.VMEM((heads, width), BF16),
            pltpu.SMEM((seqs,), jnp.int32),
            pltpu.VMEM((seqs, page_table.shape[0] // seqs), jnp.int32),
            pltpu.VMEM(key_cache.shape, BF16),
            pltpu.VMEM(value_cache.shape, BF16),
            pltpu.VMEM((n, 16, width), BF16),
            pltpu.VMEM((pages, 32, width), F32),
            pltpu.VMEM((pages, 32, width), F32),
            pltpu.VMEM((16, 32, page_len), F32),
            pltpu.VMEM((n, 16, width), F32),
            pltpu.VMEM((n, 2, width), F32),
            pltpu.VMEM((n, 16, width), F32),
            pltpu.VMEM((n, 2, width), F32),
            pltpu.VMEM((1, width), jnp.int32),
            pltpu.SMEM((1, width), jnp.int32),
            dma,
            dma,
            dma,
            dma((3,)),
            *[dma] * 8,
        ],
        compiler_params=pltpu.CompilerParams(
            collective_id=0, has_side_effects=True
        ),
    )(queries, key_cache, value_cache, key_new, value_new, lengths, page_table.reshape(seqs, -1))
    return out


def solution(mesh):
    placed = (
        P("head", "kv", None),
        P("kv", "head", None, None),
        P("kv", "head", None, None),
        P(None, "head", None),
        P(None, "head", None),
        P(),
        P(),
    )
    return jax.shard_map(
        on_device, mesh=mesh, in_specs=placed, out_specs=P("head", "kv", None), check_vma=False
    )
```

```python
import functools
import math

import jax
import jax.numpy as jnp
from jax import lax
from jax.experimental import pallas as pl
from jax.experimental.pallas import tpu as pltpu
from jax.sharding import PartitionSpec as P

LOW = -1e30
FLOOR = -5e29
F32 = jnp.float32
BF16 = jnp.bfloat16


def hops(t):
    total = 0
    while t:
        total += (0, 1, 2, 1)[t % 4]
        t //= 4
    return total


def iota(shape, dim):
    return lax.broadcasted_iota(jnp.int32, shape, dim)


def dot(a, b, dims=((1,), (0,))):
    return lax.dot_general(a, b, (dims, ((), ())), preferred_element_type=F32)


def kernel(
    n, q_hbm, k_hbm, v_hbm, kn_hbm, vn_hbm, len_hbm, tbl_hbm, out_ref,
    q_ref, kn_ref, vn_ref, len_ref, tbl_ref,
    kbuf, vbuf, qall, racc, rml, sbuf, mine, sent, meta_v, meta_s,
    ksem, vsem, qsem, insem, lsem, msem, qs_sem, qr_sem, out_sem, in_sem,
):
    pages, heads, page_len, width = kbuf.shape
    seqs = len_ref.shape[0]
    slots = tbl_ref.shape[1]
    me = lax.axis_index("kv")
    head = lax.axis_index("head")
    c = math.log2(math.e) / math.sqrt(width)
    order = sorted(range(1, n), key=hops, reverse=True)

    def peer(t):
        return (jnp.bitwise_xor(me, t), head)

    barrier = pltpu.get_barrier_semaphore()
    for t in order:
        pl.semaphore_signal(barrier, inc=1, device_id=peer(t), device_id_type=pl.DeviceIdType.MESH)

    owned = me // 2
    q_copy = pltpu.make_async_copy(q_hbm, q_ref, qsem)
    q_copy.start()
    len_copy = pltpu.make_async_copy(len_hbm, len_ref, lsem)
    len_copy.start()
    small = [
        pltpu.make_async_copy(tbl_hbm, tbl_ref, insem.at[0]),
        pltpu.make_async_copy(kn_hbm.at[owned], kn_ref, insem.at[1]),
        pltpu.make_async_copy(vn_hbm.at[owned], vn_ref, insem.at[2]),
    ]
    for one in small:
        one.start()
    q_copy.wait()
    len_copy.wait()
    for one in small:
        one.wait()
    parts = 8
    step = pages // parts
    for hbm, buf, sem in ((k_hbm, kbuf, ksem), (v_hbm, vbuf, vsem)):
        for i in range(parts):
            pltpu.make_async_copy(hbm.at[pl.ds(i * step, step)], buf.at[pl.ds(i * step, step)], sem).start()

    q16 = q_ref[...].astype(F32).reshape(16, width)
    qall[me] = q16.astype(BF16)


    rel = tbl_ref[...] - me * pages
    here = jnp.logical_and(rel >= 0, rel < pages)
    here_f = jnp.where(here, 1.0, 0.0)
    here_b = here_f.astype(BF16)
    upper = jnp.where(iota((slots, slots), 0) < iota((slots, slots), 1), 1.0, 0.0).astype(BF16)
    ones = jnp.full((slots, slots), 1.0, BF16)
    lower = jnp.where(iota((seqs, seqs), 1) < iota((seqs, seqs), 0), 1.0, 0.0).astype(BF16)
    in_row = dot(here_b, upper)
    row_total = dot(here_b, ones)
    before = dot(lower, row_total.astype(BF16))
    place = jnp.where(here, in_row + before, -1.0)
    value = ((iota((seqs, slots), 0) * slots + iota((seqs, slots), 1)) * pages + rel).astype(F32)
    value = jnp.where(here, value, 0.0)
    kth = iota((pages, slots), 0).astype(F32)
    found = jnp.zeros((pages, slots), F32)
    for s in range(seqs):
        found = found + jnp.where(place[s : s + 1] == kth, value[s : s + 1], 0.0)
    found = jnp.sum(found, axis=1, keepdims=True)
    lane = iota((pages, slots), 1)
    row = jnp.sum(jnp.where(lane == iota((pages, slots), 0), found, 0.0), axis=0, keepdims=True)
    ends = before + row_total
    lane = iota((seqs, slots), 1)
    row = row + jnp.sum(jnp.where(lane == iota((seqs, slots), 0) + pages, ends, 0.0), axis=0, keepdims=True)
    meta_v[...] = row.astype(jnp.int32)
    copy = pltpu.make_async_copy(meta_v, meta_s, msem)
    copy.start()

    row_g = iota((16, width), 0) // 4
    kn = kn_ref[...].astype(F32)
    vn = vn_ref[...].astype(F32)
    kn16 = jnp.zeros((16, width), F32)
    vn16 = jnp.zeros((16, width), F32)
    for g in range(heads):
        kn16 = jnp.where(row_g == g, kn[g : g + 1], kn16)
        vn16 = jnp.where(row_g == g, vn[g : g + 1], vn16)
    new_raw = jnp.sum(q16 * kn16, axis=1, keepdims=True)

    copy.wait()

    pl.semaphore_wait(barrier, n - 1)
    for t in order:
        pltpu.make_async_remote_copy(
            src_ref=qall.at[me], dst_ref=qall.at[me], send_sem=qs_sem, recv_sem=qr_sem,
            device_id=peer(t), device_id_type=pl.DeviceIdType.MESH,
        ).start()

    pltpu.make_async_copy(k_hbm, kbuf, ksem).wait()
    pltpu.make_async_copy(v_hbm, vbuf, vsem).wait()
    pltpu.make_async_copy(qall.at[pl.ds(0, n - 1)], qall.at[pl.ds(0, n - 1)], qr_sem).wait()

    row_group = (iota((32, width), 0) // 4) % 4
    low_half = iota((16, page_len), 0) % 8 < 4
    lanes = iota((16, page_len), 1)
    chunk = sbuf.shape[0]
    page_bits = pages.bit_length() - 1
    slot_bits = slots.bit_length() - 1

    def decode(k):
        code = meta_s[0, k]
        slot = jnp.bitwise_and(code >> page_bits, slots - 1)
        seq = jnp.bitwise_and(code >> (page_bits + slot_bits), seqs - 1)
        return jnp.bitwise_and(code, pages - 1), seq, slot

    def scores(k, pair):
        lhs, rhs = [], []
        for at in (k, k + 1):
            p, s, _ = decode(at)
            qb = qall[pl.ds(2 * s, 2)].reshape(32, width)
            none = jnp.zeros_like(qb)
            lhs.append(
                jnp.concatenate([jnp.where(row_group == 2 * pair + u, qb, none) for u in range(2)], axis=1)
            )
            rhs.append(jnp.concatenate([kbuf[p, 2 * pair], kbuf[p, 2 * pair + 1]], axis=1))
        raw = dot(jnp.concatenate(lhs, axis=0), jnp.concatenate(rhs, axis=0), ((1,), (1,)))
        a, b = 8 * pair, 16 + 8 * pair
        return (
            jnp.concatenate([raw[a : a + 8, :page_len], raw[b : b + 8, :page_len]], axis=0),
            jnp.concatenate([raw[32 + a : 40 + a, page_len:], raw[32 + b : 40 + b, page_len:]], axis=0),
        )

    def attend(k, pair, raw, state):
        m, l, acc = state
        p, s, slot = decode(k)
        before_seq = decode(jnp.maximum(k - 1, 0))[1]
        first = jnp.logical_or(k == 0, before_seq != s)
        valid = len_ref[s] - 1 - slot * page_len
        raw = jnp.where(lanes < valid, raw, LOW)
        top = jnp.maximum(jnp.max(raw, axis=1, keepdims=True), FLOOR)
        weights = jnp.exp2((raw - top) * c)
        total = jnp.sum(weights, axis=1, keepdims=True)
        lhs = jnp.concatenate(
            [jnp.where(low_half, weights, 0.0).astype(BF16), jnp.where(low_half, 0.0, weights).astype(BF16)], axis=1
        )
        page_out = dot(lhs, vbuf[p, pl.ds(2 * pair, 2)].reshape(2 * page_len, width))
        top = jnp.broadcast_to(top, m.shape)
        m = jnp.where(first, FLOOR, m)
        new_m = jnp.maximum(m, top)
        old = jnp.where(first, 0.0, jnp.exp2((m - new_m) * c))
        new = jnp.exp2((top - new_m) * c)
        l = l * old + total * new
        acc = acc * old + page_out * new
        racc[k] = acc
        rml[k] = jnp.where(lanes < 64, new_m, l)
        return new_m, l, acc

    zero = jnp.zeros((16, width), F32)
    steps = pages // chunk
    lane8 = iota((8, width), 1) % 64
    left = iota((n, width), 1) < 64
    for pair in range(2):

        def fill(i):
            for u in range(0, chunk, 2):
                sbuf[u], sbuf[u + 1] = scores(i * chunk + u, pair)

        def body(i, state):
            raws = [sbuf[u] for u in range(chunk)]
            fill(i + 1)
            for u in range(chunk):
                state = attend(i * chunk + u, pair, raws[u], state)
            return state

        fill(0)
        state = lax.fori_loop(0, steps - 1, body, (zero, zero, zero))
        for u in range(chunk):
            state = attend((steps - 1) * chunk + u, pair, sbuf[u], state)

        def gather(s, stat):
            end = meta_s[0, pages + s]
            start = jnp.where(s == 0, 0, meta_s[0, pages + jnp.maximum(s - 1, 0)])
            some = end > start
            last = jnp.clip(end - 1, 0, pages - 1)
            acc = jnp.where(some, racc[last], 0.0)
            ml = jnp.where(some, rml[last], jnp.where(lanes < 64, FLOOR, 0.0))
            mine[pair, 2 * s, 0:8] = acc[:8]
            mine[pair, 2 * s + 1, 0:8] = acc[8:]
            stat = jnp.where(lane8 == 2 * s, ml[:8], stat)
            return jnp.where(lane8 == 2 * s + 1, ml[8:], stat)

        stat = lax.fori_loop(0, seqs, gather, jnp.zeros((8, width), F32), unroll=4)
        turned = jnp.concatenate([stat] * 16, axis=0).T
        mine[pair, :, 8, :] = jnp.where(left, turned[:n], turned[n:])
        for t in order:
            pltpu.make_async_remote_copy(
                src_ref=mine.at[pair, jnp.bitwise_xor(me, t)], dst_ref=sent.at[pair, me],
                send_sem=out_sem.at[pair], recv_sem=in_sem.at[pair],
                device_id=peer(t), device_id_type=pl.DeviceIdType.MESH,
            ).start()
        sent[pair, me] = mine[pair, me]

    at_row = iota((8, width), 1) % 8 == iota((8, width), 0)
    first8 = jnp.logical_and(at_row, iota((8, width), 1) < 8)
    in_block = iota((16, width), 1) // 8 == iota((16, width), 0)
    for pair in range(2):
        some = sent.at[pair, pl.ds(0, n - 1)]
        pltpu.make_async_copy(some, some, in_sem.at[pair]).wait()
        stats = sent[pair, :, 8, :]
        turned = pltpu.roll(stats, 64, axis=1)
        tops = jnp.where(left, stats, turned)
        top = jnp.max(tops, axis=0, keepdims=True)
        w = jnp.exp2((tops - top) * c)
        total = jnp.sum(w * turned, axis=0, keepdims=True)
        top8 = jnp.sum(jnp.where(first8, top, 0.0), axis=1, keepdims=True)
        sum8 = jnp.sum(jnp.where(first8, total, 0.0), axis=1, keepdims=True)
        blocks = []
        for b in range(n // 16):
            line = jnp.sum(jnp.where(in_block, w[16 * b : 16 * b + 16], 0.0), axis=0, keepdims=True)
            blocks.append(jnp.where(at_row, line, 0.0))
        wide = jnp.concatenate(blocks, axis=1)
        wide_hi = wide.astype(BF16).astype(F32)
        lhs = jnp.concatenate([wide_hi, wide - wide_hi], axis=0).astype(BF16)
        parts = sent[pair, :, 0:8, :].reshape(8 * n, width)
        parts_hi = parts.astype(BF16)
        parts_lo = (parts - parts_hi.astype(F32)).astype(BF16)
        both = dot(lhs, parts_hi)
        numer = both[:8] + both[8:] + dot(lhs, parts_lo)[:8]
        rows = slice(8 * pair, 8 * pair + 8)
        high = jnp.maximum(top8, new_raw[rows])
        old = jnp.exp2((top8 - high) * c)
        new = jnp.exp2((new_raw[rows] - high) * c)
        result = (numer * old + new * vn16[rows]) / (sum8 * old + new)
        out_ref[2 * pair : 2 * pair + 2] = result.reshape(2, 4, width).astype(BF16)

    some = qall.at[pl.ds(0, n - 1)]
    pltpu.make_async_copy(some, some, qs_sem).wait()
    for pair in range(2):
        some = mine.at[pair, pl.ds(0, n - 1)]
        pltpu.make_async_copy(some, some, out_sem.at[pair]).wait()


def on_device(queries, key_cache, value_cache, key_new, value_new, lengths, page_table):
    n = lax.axis_size("kv")
    heads, rows, width = queries.shape
    pages, _, page_len, _ = key_cache.shape
    seqs = lengths.shape[0]
    vmem = pl.BlockSpec(memory_space=pltpu.VMEM)
    hbm = pl.BlockSpec(memory_space=pltpu.HBM)
    dma = pltpu.SemaphoreType.DMA
    out = pl.pallas_call(
        functools.partial(kernel, n),
        out_shape=jax.ShapeDtypeStruct(queries.shape, BF16),
        in_specs=[hbm] * 7,
        out_specs=vmem,
        scratch_shapes=[
            pltpu.VMEM(queries.shape, BF16),
            pltpu.VMEM((heads, width), BF16),
            pltpu.VMEM((heads, width), BF16),
            pltpu.SMEM((seqs,), jnp.int32),
            pltpu.VMEM((seqs, page_table.shape[0] // seqs), jnp.int32),
            pltpu.VMEM(key_cache.shape, BF16),
            pltpu.VMEM(value_cache.shape, BF16),
            pltpu.VMEM((n, 16, width), BF16),
            pltpu.VMEM((pages, 16, width), F32),
            pltpu.VMEM((pages, 16, width), F32),
            pltpu.VMEM((16, 16, page_len), F32),
            pltpu.VMEM((2, n, 9, width), F32),
            pltpu.VMEM((2, n, 9, width), F32),
            pltpu.VMEM((1, width), jnp.int32),
            pltpu.SMEM((1, width), jnp.int32),
            dma,
            dma,
            dma,
            dma((3,)),
            *[dma] * 4,
            dma((2,)),
            dma((2,)),
        ],
        compiler_params=pltpu.CompilerParams(
            collective_id=0, has_side_effects=True
        ),
    )(queries, key_cache, value_cache, key_new, value_new, lengths, page_table.reshape(seqs, -1))
    return out


def solution(mesh):
    placed = (
        P("head", "kv", None),
        P("kv", "head", None, None),
        P("kv", "head", None, None),
        P(None, "head", None),
        P(None, "head", None),
        P(),
        P(),
    )
    return jax.shard_map(
        on_device, mesh=mesh, in_specs=placed, out_specs=P("head", "kv", None), check_vma=False
    )
```

```python
import functools
import math

import jax
import jax.numpy as jnp
from jax import lax
from jax.experimental import pallas as pl
from jax.experimental.pallas import tpu as pltpu
from jax.sharding import PartitionSpec as P

LOW = -1e30
FLOOR = -5e29
F32 = jnp.float32
BF16 = jnp.bfloat16


def hops(t):
    total = 0
    while t:
        total += (0, 1, 2, 1)[t % 4]
        t //= 4
    return total


def iota(shape, dim):
    return lax.broadcasted_iota(jnp.int32, shape, dim)


def dot(a, b, dims=((1,), (0,))):
    return lax.dot_general(a, b, (dims, ((), ())), preferred_element_type=F32)


def kernel(
    n, q_hbm, k_hbm, v_hbm, kn_hbm, vn_hbm, len_hbm, tbl_hbm, out_ref,
    q_ref, kn_ref, vn_ref, len_ref, tbl_ref,
    kbuf, vbuf, qall, racc, rml, sbuf, mine, sent, meta_v, meta_s,
    ksem, vsem, qsem, insem, lsem, msem, qs_sem, qr_sem, out_sem, in_sem,
):
    pages, heads, page_len, width = kbuf.shape
    seqs = len_ref.shape[0]
    slots = tbl_ref.shape[1]
    me = lax.axis_index("kv")
    head = lax.axis_index("head")
    c = math.log2(math.e) / math.sqrt(width)
    order = sorted(range(1, n), key=hops, reverse=True)

    def peer(t):
        return (jnp.bitwise_xor(me, t), head)

    barrier = pltpu.get_barrier_semaphore()
    for t in order:
        pl.semaphore_signal(barrier, inc=1, device_id=peer(t), device_id_type=pl.DeviceIdType.MESH)

    owned = me // 2
    q_copy = pltpu.make_async_copy(q_hbm, q_ref, qsem)
    q_copy.start()
    len_copy = pltpu.make_async_copy(len_hbm, len_ref, lsem)
    len_copy.start()
    small = [
        pltpu.make_async_copy(tbl_hbm, tbl_ref, insem.at[0]),
        pltpu.make_async_copy(kn_hbm.at[owned], kn_ref, insem.at[1]),
        pltpu.make_async_copy(vn_hbm.at[owned], vn_ref, insem.at[2]),
    ]
    for one in small:
        one.start()
    q_copy.wait()
    len_copy.wait()
    for one in small:
        one.wait()
    parts = 8
    step = pages // parts
    for hbm, buf, sem in ((k_hbm, kbuf, ksem), (v_hbm, vbuf, vsem)):
        for i in range(parts):
            pltpu.make_async_copy(hbm.at[pl.ds(i * step, step)], buf.at[pl.ds(i * step, step)], sem).start()

    q16 = q_ref[...].astype(F32).reshape(16, width)
    qall[me] = q16.astype(BF16)


    rel = tbl_ref[...] - me * pages
    here = jnp.logical_and(rel >= 0, rel < pages)
    here_f = jnp.where(here, 1.0, 0.0)
    here_b = here_f.astype(BF16)
    upper = jnp.where(iota((slots, slots), 0) < iota((slots, slots), 1), 1.0, 0.0).astype(BF16)
    ones = jnp.full((slots, slots), 1.0, BF16)
    lower = jnp.where(iota((seqs, seqs), 1) < iota((seqs, seqs), 0), 1.0, 0.0).astype(BF16)
    in_row = dot(here_b, upper)
    row_total = dot(here_b, ones)
    before = dot(lower, row_total.astype(BF16))
    place = jnp.where(here, in_row + before, -1.0)
    value = ((iota((seqs, slots), 0) * slots + iota((seqs, slots), 1)) * pages + rel).astype(F32)
    value = jnp.where(here, value, 0.0)
    kth = iota((pages, slots), 0).astype(F32)
    found = jnp.zeros((pages, slots), F32)
    for s in range(seqs):
        found = found + jnp.where(place[s : s + 1] == kth, value[s : s + 1], 0.0)
    found = jnp.sum(found, axis=1, keepdims=True)
    lane = iota((pages, slots), 1)
    row = jnp.sum(jnp.where(lane == iota((pages, slots), 0), found, 0.0), axis=0, keepdims=True)
    ends = before + row_total
    lane = iota((seqs, slots), 1)
    row = row + jnp.sum(jnp.where(lane == iota((seqs, slots), 0) + pages, ends, 0.0), axis=0, keepdims=True)
    meta_v[...] = row.astype(jnp.int32)
    copy = pltpu.make_async_copy(meta_v, meta_s, msem)
    copy.start()

    row_g = iota((16, width), 0) // 4
    kn = kn_ref[...].astype(F32)
    vn = vn_ref[...].astype(F32)
    kn16 = jnp.zeros((16, width), F32)
    vn16 = jnp.zeros((16, width), F32)
    for g in range(heads):
        kn16 = jnp.where(row_g == g, kn[g : g + 1], kn16)
        vn16 = jnp.where(row_g == g, vn[g : g + 1], vn16)
    new_raw = jnp.sum(q16 * kn16, axis=1, keepdims=True)

    copy.wait()

    pl.semaphore_wait(barrier, n - 1)
    for t in order:
        pltpu.make_async_remote_copy(
            src_ref=qall.at[me], dst_ref=qall.at[me], send_sem=qs_sem, recv_sem=qr_sem,
            device_id=peer(t), device_id_type=pl.DeviceIdType.MESH,
        ).start()

    pltpu.make_async_copy(k_hbm, kbuf, ksem).wait()
    pltpu.make_async_copy(v_hbm, vbuf, vsem).wait()
    pltpu.make_async_copy(qall.at[pl.ds(0, n - 1)], qall.at[pl.ds(0, n - 1)], qr_sem).wait()

    row_group = (iota((32, width), 0) // 4) % 4
    low_half = iota((16, page_len), 0) % 8 < 4
    lanes = iota((16, page_len), 1)
    chunk = sbuf.shape[0]
    page_bits = pages.bit_length() - 1
    slot_bits = slots.bit_length() - 1

    def decode(k):
        code = meta_s[0, k]
        slot = jnp.bitwise_and(code >> page_bits, slots - 1)
        seq = jnp.bitwise_and(code >> (page_bits + slot_bits), seqs - 1)
        return jnp.bitwise_and(code, pages - 1), seq, slot

    def scores(k, pair):
        lhs, rhs = [], []
        for at in (k, k + 1):
            p, s, _ = decode(at)
            qb = qall[pl.ds(2 * s, 2)].reshape(32, width)
            none = jnp.zeros_like(qb)
            lhs.append(
                jnp.concatenate([jnp.where(row_group == 2 * pair + u, qb, none) for u in range(2)], axis=1)
            )
            rhs.append(jnp.concatenate([kbuf[p, 2 * pair], kbuf[p, 2 * pair + 1]], axis=1))
        raw = dot(jnp.concatenate(lhs, axis=0), jnp.concatenate(rhs, axis=0), ((1,), (1,)))
        a, b = 8 * pair, 16 + 8 * pair
        return (
            jnp.concatenate([raw[a : a + 8, :page_len], raw[b : b + 8, :page_len]], axis=0),
            jnp.concatenate([raw[32 + a : 40 + a, page_len:], raw[32 + b : 40 + b, page_len:]], axis=0),
        )

    def attend(k, pair, raw, state):
        m, l, acc = state
        p, s, slot = decode(k)
        before_seq = decode(jnp.maximum(k - 1, 0))[1]
        first = jnp.logical_or(k == 0, before_seq != s)
        valid = len_ref[s] - 1 - slot * page_len
        raw = jnp.where(lanes < valid, raw, LOW)
        top = jnp.maximum(jnp.max(raw, axis=1, keepdims=True), FLOOR)
        weights = jnp.exp2((raw - top) * c)
        total = jnp.sum(weights, axis=1, keepdims=True)
        lhs = jnp.concatenate(
            [jnp.where(low_half, weights, 0.0).astype(BF16), jnp.where(low_half, 0.0, weights).astype(BF16)], axis=1
        )
        page_out = dot(lhs, vbuf[p, pl.ds(2 * pair, 2)].reshape(2 * page_len, width))
        top = jnp.broadcast_to(top, m.shape)
        m = jnp.where(first, FLOOR, m)
        new_m = jnp.maximum(m, top)
        old = jnp.where(first, 0.0, jnp.exp2((m - new_m) * c))
        new = jnp.exp2((top - new_m) * c)
        l = l * old + total * new
        acc = acc * old + page_out * new
        racc[k] = acc
        rml[k] = jnp.where(lanes < 64, new_m, l)
        return new_m, l, acc

    zero = jnp.zeros((16, width), F32)
    steps = pages // chunk
    lane8 = iota((8, width), 1) % 64
    left = iota((n, width), 1) < 64
    for pair in range(2):

        def fill(i):
            for u in range(0, chunk, 2):
                sbuf[u], sbuf[u + 1] = scores(i * chunk + u, pair)

        def body(i, state):
            raws = [sbuf[u] for u in range(chunk)]
            fill(i + 1)
            for u in range(chunk):
                state = attend(i * chunk + u, pair, raws[u], state)
            return state

        fill(0)
        state = lax.fori_loop(0, steps - 1, body, (zero, zero, zero))
        for u in range(chunk):
            state = attend((steps - 1) * chunk + u, pair, sbuf[u], state)

        def gather(s, stat):
            end = meta_s[0, pages + s]
            start = jnp.where(s == 0, 0, meta_s[0, pages + jnp.maximum(s - 1, 0)])
            some = end > start
            last = jnp.clip(end - 1, 0, pages - 1)
            acc = jnp.where(some, racc[last], 0.0)
            ml = jnp.where(some, rml[last], jnp.where(lanes < 64, FLOOR, 0.0))
            mine[pair, 2 * s, 0:8] = acc[:8]
            mine[pair, 2 * s + 1, 0:8] = acc[8:]
            stat = jnp.where(lane8 == 2 * s, ml[:8], stat)
            return jnp.where(lane8 == 2 * s + 1, ml[8:], stat)

        stat = lax.fori_loop(0, seqs, gather, jnp.zeros((8, width), F32), unroll=4)
        turned = jnp.concatenate([stat] * 16, axis=0).T
        mine[pair, :, 8, :] = jnp.where(left, turned[:n], turned[n:])
        for t in order:
            pltpu.make_async_remote_copy(
                src_ref=mine.at[pair, jnp.bitwise_xor(me, t)], dst_ref=sent.at[pair, me],
                send_sem=out_sem.at[pair], recv_sem=in_sem.at[pair],
                device_id=peer(t), device_id_type=pl.DeviceIdType.MESH,
            ).start()
        sent[pair, me] = mine[pair, me]

    at_row = iota((8, width), 1) % 8 == iota((8, width), 0)
    first8 = jnp.logical_and(at_row, iota((8, width), 1) < 8)
    in_block = iota((16, width), 1) // 8 == iota((16, width), 0)
    for pair in range(2):
        some = sent.at[pair, pl.ds(0, n - 1)]
        pltpu.make_async_copy(some, some, in_sem.at[pair]).wait()
        stats = sent[pair, :, 8, :]
        turned = pltpu.roll(stats, 64, axis=1)
        tops = jnp.where(left, stats, turned)
        top = jnp.max(tops, axis=0, keepdims=True)
        w = jnp.exp2((tops - top) * c)
        total = jnp.sum(w * turned, axis=0, keepdims=True)
        top8 = jnp.sum(jnp.where(first8, top, 0.0), axis=1, keepdims=True)
        sum8 = jnp.sum(jnp.where(first8, total, 0.0), axis=1, keepdims=True)
        blocks = []
        for b in range(n // 16):
            line = jnp.sum(jnp.where(in_block, w[16 * b : 16 * b + 16], 0.0), axis=0, keepdims=True)
            blocks.append(jnp.where(at_row, line, 0.0))
        wide = jnp.concatenate(blocks, axis=1)
        wide_hi = wide.astype(BF16).astype(F32)
        lhs = jnp.concatenate([wide_hi, wide - wide_hi], axis=0).astype(BF16)
        parts = sent[pair, :, 0:8, :].reshape(8 * n, width)
        parts_hi = parts.astype(BF16)
        parts_lo = (parts - parts_hi.astype(F32)).astype(BF16)
        both = dot(lhs, parts_hi)
        numer = both[:8] + both[8:] + dot(lhs, parts_lo)[:8]
        rows = slice(8 * pair, 8 * pair + 8)
        high = jnp.maximum(top8, new_raw[rows])
        old = jnp.exp2((top8 - high) * c)
        new = jnp.exp2((new_raw[rows] - high) * c)
        result = (numer * old + new * vn16[rows]) / (sum8 * old + new)
        out_ref[rows] = result

    some = qall.at[pl.ds(0, n - 1)]
    pltpu.make_async_copy(some, some, qs_sem).wait()
    for pair in range(2):
        some = mine.at[pair, pl.ds(0, n - 1)]
        pltpu.make_async_copy(some, some, out_sem.at[pair]).wait()


def on_device(queries, key_cache, value_cache, key_new, value_new, lengths, page_table):
    n = lax.axis_size("kv")
    heads, rows, width = queries.shape
    pages, _, page_len, _ = key_cache.shape
    seqs = lengths.shape[0]
    vmem = pl.BlockSpec(memory_space=pltpu.VMEM)
    hbm = pl.BlockSpec(memory_space=pltpu.HBM)
    dma = pltpu.SemaphoreType.DMA
    inputs = (queries, key_cache, value_cache, key_new, value_new, lengths, page_table.reshape(seqs, -1))
    out = pl.pallas_call(
        functools.partial(kernel, n),
        out_shape=jax.ShapeDtypeStruct((heads * rows, width), F32),
        in_specs=[hbm] * 7,
        out_specs=vmem,
        scratch_shapes=[
            pltpu.VMEM(queries.shape, BF16),
            pltpu.VMEM((heads, width), BF16),
            pltpu.VMEM((heads, width), BF16),
            pltpu.SMEM((seqs,), jnp.int32),
            pltpu.VMEM((seqs, page_table.shape[0] // seqs), jnp.int32),
            pltpu.VMEM(key_cache.shape, BF16),
            pltpu.VMEM(value_cache.shape, BF16),
            pltpu.VMEM((n, 16, width), BF16),
            pltpu.VMEM((pages, 16, width), F32),
            pltpu.VMEM((pages, 16, width), F32),
            pltpu.VMEM((16, 16, page_len), F32),
            pltpu.VMEM((2, n, 9, width), F32),
            pltpu.VMEM((2, n, 9, width), F32),
            pltpu.VMEM((1, width), jnp.int32),
            pltpu.SMEM((1, width), jnp.int32),
            dma,
            dma,
            dma,
            dma((3,)),
            *[dma] * 4,
            dma((2,)),
            dma((2,)),
        ],
        compiler_params=pltpu.CompilerParams(
            collective_id=0, has_side_effects=True, vmem_limit_bytes=48 * 1024 * 1024
        ),
    )(*(pltpu.with_memory_space_constraint(x, pltpu.HBM) for x in inputs))
    return out.reshape(heads, rows, width).astype(BF16)


def solution(mesh):
    placed = (
        P("head", "kv", None),
        P("kv", "head", None, None),
        P("kv", "head", None, None),
        P(None, "head", None),
        P(None, "head", None),
        P(),
        P(),
    )
    return jax.shard_map(
        on_device, mesh=mesh, in_specs=placed, out_specs=P("head", "kv", None), check_vma=False
    )
```

```python
import functools
import math

import jax
import jax.numpy as jnp
from jax import lax
from jax.experimental import pallas as pl
from jax.experimental.pallas import tpu as pltpu
from jax.sharding import PartitionSpec as P

UNROLL = 4
LOW = -1e30
FLOOR = -5e29
F32 = jnp.float32
BF16 = jnp.bfloat16


def hops(t):
    total = 0
    while t:
        total += (0, 1, 2, 1)[t % 4]
        t //= 4
    return total


def iota(shape, dim):
    return lax.broadcasted_iota(jnp.int32, shape, dim)


def dot(a, b, dims=((1,), (0,))):
    return lax.dot_general(a, b, (dims, ((), ())), preferred_element_type=F32)


def kernel(
    n, q_hbm, k_hbm, v_hbm, kn_hbm, vn_hbm, len_hbm, tbl_hbm, out_ref,
    q_ref, kn_ref, vn_ref, len_ref, tbl_ref,
    kbuf, vbuf, qall, racc, rml, sbuf, mine, sent, meta_v, meta_s,
    ksem, vsem, qsem, insem, lsem, msem, qs_sem, qr_sem, out_sem, in_sem,
):
    pages, heads, page_len, width = kbuf.shape
    seqs = len_ref.shape[0]
    slots = tbl_ref.shape[1]
    me = lax.axis_index("kv")
    head = lax.axis_index("head")
    c = math.log2(math.e) / math.sqrt(width)
    order = sorted(range(1, n), key=hops, reverse=True)

    def peer(t):
        return (jnp.bitwise_xor(me, t), head)

    barrier = pltpu.get_barrier_semaphore()
    for t in order:
        pl.semaphore_signal(barrier, inc=1, device_id=peer(t), device_id_type=pl.DeviceIdType.MESH)

    owned = me // 2
    q_copy = pltpu.make_async_copy(q_hbm, q_ref, qsem)
    q_copy.start()
    len_copy = pltpu.make_async_copy(len_hbm, len_ref, lsem)
    len_copy.start()
    small = [
        pltpu.make_async_copy(tbl_hbm, tbl_ref, insem.at[0]),
        pltpu.make_async_copy(kn_hbm.at[owned], kn_ref, insem.at[1]),
        pltpu.make_async_copy(vn_hbm.at[owned], vn_ref, insem.at[2]),
    ]
    for one in small:
        one.start()
    q_copy.wait()
    len_copy.wait()
    for one in small:
        one.wait()
    parts = 8
    step = pages // parts
    for hbm, buf, sem in ((k_hbm, kbuf, ksem), (v_hbm, vbuf, vsem)):
        for i in range(parts):
            pltpu.make_async_copy(hbm.at[pl.ds(i * step, step)], buf.at[pl.ds(i * step, step)], sem).start()

    q16 = q_ref[...].astype(F32).reshape(16, width)
    qall[me] = q16.astype(BF16)


    rel = tbl_ref[...] - me * pages
    here = jnp.logical_and(rel >= 0, rel < pages)
    here_f = jnp.where(here, 1.0, 0.0)
    here_b = here_f.astype(BF16)
    upper = jnp.where(iota((slots, slots), 0) < iota((slots, slots), 1), 1.0, 0.0).astype(BF16)
    ones = jnp.full((slots, slots), 1.0, BF16)
    lower = jnp.where(iota((seqs, seqs), 1) < iota((seqs, seqs), 0), 1.0, 0.0).astype(BF16)
    in_row = dot(here_b, upper)
    row_total = dot(here_b, ones)
    before = dot(lower, row_total.astype(BF16))
    place = jnp.where(here, in_row + before, -1.0)
    value = ((iota((seqs, slots), 0) * slots + iota((seqs, slots), 1)) * pages + rel).astype(F32)
    value = jnp.where(here, value, 0.0)
    kth = iota((pages, slots), 0).astype(F32)
    found = jnp.zeros((pages, slots), F32)
    for s in range(seqs):
        found = found + jnp.where(place[s : s + 1] == kth, value[s : s + 1], 0.0)
    found = jnp.sum(found, axis=1, keepdims=True)
    lane = iota((pages, slots), 1)
    row = jnp.sum(jnp.where(lane == iota((pages, slots), 0), found, 0.0), axis=0, keepdims=True)
    ends = before + row_total
    lane = iota((seqs, slots), 1)
    row = row + jnp.sum(jnp.where(lane == iota((seqs, slots), 0) + pages, ends, 0.0), axis=0, keepdims=True)
    meta_v[...] = row.astype(jnp.int32)
    copy = pltpu.make_async_copy(meta_v, meta_s, msem)
    copy.start()

    row_g = iota((16, width), 0) // 4
    kn = kn_ref[...].astype(F32)
    vn = vn_ref[...].astype(F32)
    kn16 = jnp.zeros((16, width), F32)
    vn16 = jnp.zeros((16, width), F32)
    for g in range(heads):
        kn16 = jnp.where(row_g == g, kn[g : g + 1], kn16)
        vn16 = jnp.where(row_g == g, vn[g : g + 1], vn16)
    new_raw = jnp.sum(q16 * kn16, axis=1, keepdims=True)

    copy.wait()

    pl.semaphore_wait(barrier, n - 1)
    for t in order:
        pltpu.make_async_remote_copy(
            src_ref=qall.at[me], dst_ref=qall.at[me], send_sem=qs_sem, recv_sem=qr_sem,
            device_id=peer(t), device_id_type=pl.DeviceIdType.MESH,
        ).start()

    pltpu.make_async_copy(k_hbm, kbuf, ksem).wait()

    def turn(p, carry):
        for g in range(heads):
            kbuf[p, g] = kbuf[p, g].T
        return carry

    lax.fori_loop(0, pages, turn, 0, unroll=UNROLL)
    pltpu.make_async_copy(v_hbm, vbuf, vsem).wait()
    pltpu.make_async_copy(qall.at[pl.ds(0, n - 1)], qall.at[pl.ds(0, n - 1)], qr_sem).wait()

    row_group = (iota((32, width), 0) // 4) % 4
    low_half = iota((16, page_len), 0) % 8 < 4
    lanes = iota((16, page_len), 1)
    chunk = sbuf.shape[0]
    page_bits = pages.bit_length() - 1
    slot_bits = slots.bit_length() - 1

    def decode(k):
        code = meta_s[0, k]
        slot = jnp.bitwise_and(code >> page_bits, slots - 1)
        seq = jnp.bitwise_and(code >> (page_bits + slot_bits), seqs - 1)
        return jnp.bitwise_and(code, pages - 1), seq, slot

    def scores(k, pair):
        lhs, rhs = [], []
        for at in (k, k + 1):
            p, s, _ = decode(at)
            qb = qall[pl.ds(2 * s, 2)].reshape(32, width)
            none = jnp.zeros_like(qb)
            lhs.append(
                jnp.concatenate([jnp.where(row_group == 2 * pair + u, qb, none) for u in range(2)], axis=1)
            )
            rhs.append(kbuf[p, pl.ds(2 * pair, 2)].reshape(2 * width, page_len))
        raw = dot(jnp.concatenate(lhs, axis=0), jnp.concatenate(rhs, axis=1))
        a, b = 8 * pair, 16 + 8 * pair
        return (
            jnp.concatenate([raw[a : a + 8, :page_len], raw[b : b + 8, :page_len]], axis=0),
            jnp.concatenate([raw[32 + a : 40 + a, page_len:], raw[32 + b : 40 + b, page_len:]], axis=0),
        )

    def attend(k, pair, raw, state):
        m, l, acc = state
        p, s, slot = decode(k)
        before_seq = decode(jnp.maximum(k - 1, 0))[1]
        first = jnp.logical_or(k == 0, before_seq != s)
        valid = len_ref[s] - 1 - slot * page_len
        raw = jnp.where(lanes < valid, raw, LOW)
        top = jnp.maximum(jnp.max(raw, axis=1, keepdims=True), FLOOR)
        weights = jnp.exp2((raw - top) * c)
        total = jnp.sum(weights, axis=1, keepdims=True)
        lhs = jnp.concatenate(
            [jnp.where(low_half, weights, 0.0).astype(BF16), jnp.where(low_half, 0.0, weights).astype(BF16)], axis=1
        )
        page_out = dot(lhs, vbuf[p, pl.ds(2 * pair, 2)].reshape(2 * page_len, width))
        top = jnp.broadcast_to(top, m.shape)
        m = jnp.where(first, FLOOR, m)
        new_m = jnp.maximum(m, top)
        old = jnp.where(first, 0.0, jnp.exp2((m - new_m) * c))
        new = jnp.exp2((top - new_m) * c)
        l = l * old + total * new
        acc = acc * old + page_out * new
        racc[k] = acc
        rml[k] = jnp.where(lanes < 64, new_m, l)
        return new_m, l, acc

    zero = jnp.zeros((16, width), F32)
    steps = pages // chunk
    lane8 = iota((8, width), 1) % 64
    left = iota((n, width), 1) < 64
    for pair in range(2):

        def fill(i):
            for u in range(0, chunk, 2):
                sbuf[u], sbuf[u + 1] = scores(i * chunk + u, pair)

        def body(i, state):
            raws = [sbuf[u] for u in range(chunk)]
            fill(i + 1)
            for u in range(chunk):
                state = attend(i * chunk + u, pair, raws[u], state)
            return state

        fill(0)
        state = lax.fori_loop(0, steps - 1, body, (zero, zero, zero))
        for u in range(chunk):
            state = attend((steps - 1) * chunk + u, pair, sbuf[u], state)

        def gather(s, stat):
            end = meta_s[0, pages + s]
            start = jnp.where(s == 0, 0, meta_s[0, pages + jnp.maximum(s - 1, 0)])
            some = end > start
            last = jnp.clip(end - 1, 0, pages - 1)
            acc = jnp.where(some, racc[last], 0.0)
            ml = jnp.where(some, rml[last], jnp.where(lanes < 64, FLOOR, 0.0))
            mine[pair, 2 * s, 0:8] = acc[:8]
            mine[pair, 2 * s + 1, 0:8] = acc[8:]
            stat = jnp.where(lane8 == 2 * s, ml[:8], stat)
            return jnp.where(lane8 == 2 * s + 1, ml[8:], stat)

        stat = lax.fori_loop(0, seqs, gather, jnp.zeros((8, width), F32), unroll=4)
        turned = jnp.concatenate([stat] * 16, axis=0).T
        mine[pair, :, 8, :] = jnp.where(left, turned[:n], turned[n:])
        for t in order:
            pltpu.make_async_remote_copy(
                src_ref=mine.at[pair, jnp.bitwise_xor(me, t)], dst_ref=sent.at[pair, me],
                send_sem=out_sem.at[pair], recv_sem=in_sem.at[pair],
                device_id=peer(t), device_id_type=pl.DeviceIdType.MESH,
            ).start()
        sent[pair, me] = mine[pair, me]

    at_row = iota((8, width), 1) % 8 == iota((8, width), 0)
    first8 = jnp.logical_and(at_row, iota((8, width), 1) < 8)
    in_block = iota((16, width), 1) // 8 == iota((16, width), 0)
    for pair in range(2):
        some = sent.at[pair, pl.ds(0, n - 1)]
        pltpu.make_async_copy(some, some, in_sem.at[pair]).wait()
        stats = sent[pair, :, 8, :]
        turned = pltpu.roll(stats, 64, axis=1)
        tops = jnp.where(left, stats, turned)
        top = jnp.max(tops, axis=0, keepdims=True)
        w = jnp.exp2((tops - top) * c)
        total = jnp.sum(w * turned, axis=0, keepdims=True)
        top8 = jnp.sum(jnp.where(first8, top, 0.0), axis=1, keepdims=True)
        sum8 = jnp.sum(jnp.where(first8, total, 0.0), axis=1, keepdims=True)
        blocks = []
        for b in range(n // 16):
            line = jnp.sum(jnp.where(in_block, w[16 * b : 16 * b + 16], 0.0), axis=0, keepdims=True)
            blocks.append(jnp.where(at_row, line, 0.0))
        wide = jnp.concatenate(blocks, axis=1)
        wide_hi = wide.astype(BF16).astype(F32)
        lhs = jnp.concatenate([wide_hi, wide - wide_hi], axis=0).astype(BF16)
        parts = sent[pair, :, 0:8, :].reshape(8 * n, width)
        parts_hi = parts.astype(BF16)
        parts_lo = (parts - parts_hi.astype(F32)).astype(BF16)
        both = dot(lhs, parts_hi)
        numer = both[:8] + both[8:] + dot(lhs, parts_lo)[:8]
        rows = slice(8 * pair, 8 * pair + 8)
        high = jnp.maximum(top8, new_raw[rows])
        old = jnp.exp2((top8 - high) * c)
        new = jnp.exp2((new_raw[rows] - high) * c)
        result = (numer * old + new * vn16[rows]) / (sum8 * old + new)
        out_ref[rows] = result

    some = qall.at[pl.ds(0, n - 1)]
    pltpu.make_async_copy(some, some, qs_sem).wait()
    for pair in range(2):
        some = mine.at[pair, pl.ds(0, n - 1)]
        pltpu.make_async_copy(some, some, out_sem.at[pair]).wait()


def on_device(queries, key_cache, value_cache, key_new, value_new, lengths, page_table):
    n = lax.axis_size("kv")
    heads, rows, width = queries.shape
    pages, _, page_len, _ = key_cache.shape
    seqs = lengths.shape[0]
    vmem = pl.BlockSpec(memory_space=pltpu.VMEM)
    hbm = pl.BlockSpec(memory_space=pltpu.HBM)
    dma = pltpu.SemaphoreType.DMA
    inputs = (queries, key_cache, value_cache, key_new, value_new, lengths, page_table.reshape(seqs, -1))
    out = pl.pallas_call(
        functools.partial(kernel, n),
        out_shape=jax.ShapeDtypeStruct((heads * rows, width), F32),
        in_specs=[hbm] * 7,
        out_specs=vmem,
        scratch_shapes=[
            pltpu.VMEM(queries.shape, BF16),
            pltpu.VMEM((heads, width), BF16),
            pltpu.VMEM((heads, width), BF16),
            pltpu.SMEM((seqs,), jnp.int32),
            pltpu.VMEM((seqs, page_table.shape[0] // seqs), jnp.int32),
            pltpu.VMEM(key_cache.shape, BF16),
            pltpu.VMEM(value_cache.shape, BF16),
            pltpu.VMEM((n, 16, width), BF16),
            pltpu.VMEM((pages, 16, width), F32),
            pltpu.VMEM((pages, 16, width), F32),
            pltpu.VMEM((32, 16, page_len), F32),
            pltpu.VMEM((2, n, 9, width), F32),
            pltpu.VMEM((2, n, 9, width), F32),
            pltpu.VMEM((1, width), jnp.int32),
            pltpu.SMEM((1, width), jnp.int32),
            dma,
            dma,
            dma,
            dma((3,)),
            *[dma] * 4,
            dma((2,)),
            dma((2,)),
        ],
        compiler_params=pltpu.CompilerParams(
            collective_id=0, has_side_effects=True, vmem_limit_bytes=48 * 1024 * 1024
        ),
    )(*(pltpu.with_memory_space_constraint(x, pltpu.HBM) for x in inputs))
    return out.reshape(heads, rows, width).astype(BF16)


def solution(mesh):
    placed = (
        P("head", "kv", None),
        P("kv", "head", None, None),
        P("kv", "head", None, None),
        P(None, "head", None),
        P(None, "head", None),
        P(),
        P(),
    )
    return jax.shard_map(
        on_device, mesh=mesh, in_specs=placed, out_specs=P("head", "kv", None), check_vma=False
    )
```

```python
import functools
import math

import jax
import jax.numpy as jnp
from jax import lax
from jax.experimental import pallas as pl
from jax.experimental.pallas import tpu as pltpu
from jax.sharding import PartitionSpec as P

UNROLL = 4
LOW = -1e30
FLOOR = -5e29
F32 = jnp.float32
BF16 = jnp.bfloat16


def hops(t):
    total = 0
    while t:
        total += (0, 1, 2, 1)[t % 4]
        t //= 4
    return total


def iota(shape, dim):
    return lax.broadcasted_iota(jnp.int32, shape, dim)


def dot(a, b, dims=((1,), (0,))):
    return lax.dot_general(a, b, (dims, ((), ())), preferred_element_type=F32)


def kernel(
    n, q_hbm, k_hbm, v_hbm, kn_hbm, vn_hbm, len_hbm, tbl_hbm, out_ref,
    q_ref, kn_ref, vn_ref, len_ref, tbl_ref,
    kbuf, vbuf, qall, racc, rml, sbuf, mine, sent, meta_v, meta_s,
    ksem, vsem, qsem, insem, lsem, msem, qs_sem, qr_sem, out_sem, in_sem,
):
    pages, heads, page_len, width = kbuf.shape
    seqs = len_ref.shape[0]
    slots = tbl_ref.shape[1]
    me = lax.axis_index("kv")
    head = lax.axis_index("head")
    c = math.log2(math.e) / math.sqrt(width)
    order = sorted(range(1, n), key=hops, reverse=True)

    def peer(t):
        return (jnp.bitwise_xor(me, t), head)

    barrier = pltpu.get_barrier_semaphore()
    for t in order:
        pl.semaphore_signal(barrier, inc=1, device_id=peer(t), device_id_type=pl.DeviceIdType.MESH)

    owned = me // 2
    q_copy = pltpu.make_async_copy(q_hbm, q_ref, qsem)
    q_copy.start()
    len_copy = pltpu.make_async_copy(len_hbm, len_ref, lsem)
    len_copy.start()
    small = [
        pltpu.make_async_copy(tbl_hbm, tbl_ref, insem.at[0]),
        pltpu.make_async_copy(kn_hbm.at[owned], kn_ref, insem.at[1]),
        pltpu.make_async_copy(vn_hbm.at[owned], vn_ref, insem.at[2]),
    ]
    for one in small:
        one.start()
    q_copy.wait()
    len_copy.wait()
    for one in small:
        one.wait()
    parts = 8
    step = pages // parts
    for hbm, buf, sem in ((k_hbm, kbuf, ksem), (v_hbm, vbuf, vsem)):
        for i in range(parts):
            pltpu.make_async_copy(hbm.at[pl.ds(i * step, step)], buf.at[pl.ds(i * step, step)], sem).start()

    q16 = q_ref[...].astype(F32).reshape(16, width)
    qall[me] = q16.astype(BF16)


    rel = tbl_ref[...] - me * pages
    here = jnp.logical_and(rel >= 0, rel < pages)
    here_f = jnp.where(here, 1.0, 0.0)
    here_b = here_f.astype(BF16)
    upper = jnp.where(iota((slots, slots), 0) < iota((slots, slots), 1), 1.0, 0.0).astype(BF16)
    ones = jnp.full((slots, slots), 1.0, BF16)
    lower = jnp.where(iota((seqs, seqs), 1) < iota((seqs, seqs), 0), 1.0, 0.0).astype(BF16)
    in_row = dot(here_b, upper)
    row_total = dot(here_b, ones)
    before = dot(lower, row_total.astype(BF16))
    place = jnp.where(here, in_row + before, -1.0)
    value = ((iota((seqs, slots), 0) * slots + iota((seqs, slots), 1)) * pages + rel).astype(F32)
    value = jnp.where(here, value, 0.0)
    kth = iota((pages, slots), 0).astype(F32)
    found = jnp.zeros((pages, slots), F32)
    for s in range(seqs):
        found = found + jnp.where(place[s : s + 1] == kth, value[s : s + 1], 0.0)
    found = jnp.sum(found, axis=1, keepdims=True)
    lane = iota((pages, slots), 1)
    row = jnp.sum(jnp.where(lane == iota((pages, slots), 0), found, 0.0), axis=0, keepdims=True)
    ends = before + row_total
    lane = iota((seqs, slots), 1)
    row = row + jnp.sum(jnp.where(lane == iota((seqs, slots), 0) + pages, ends, 0.0), axis=0, keepdims=True)
    meta_v[...] = row.astype(jnp.int32)
    copy = pltpu.make_async_copy(meta_v, meta_s, msem)
    copy.start()

    row_g = iota((16, width), 0) // 4
    kn = kn_ref[...].astype(F32)
    vn = vn_ref[...].astype(F32)
    kn16 = jnp.zeros((16, width), F32)
    vn16 = jnp.zeros((16, width), F32)
    for g in range(heads):
        kn16 = jnp.where(row_g == g, kn[g : g + 1], kn16)
        vn16 = jnp.where(row_g == g, vn[g : g + 1], vn16)
    new_raw = jnp.sum(q16 * kn16, axis=1, keepdims=True)

    copy.wait()

    pl.semaphore_wait(barrier, n - 1)
    for t in order:
        pltpu.make_async_remote_copy(
            src_ref=qall.at[me], dst_ref=qall.at[me], send_sem=qs_sem, recv_sem=qr_sem,
            device_id=peer(t), device_id_type=pl.DeviceIdType.MESH,
        ).start()

    pltpu.make_async_copy(k_hbm, kbuf, ksem).wait()

    def turn(p, carry):
        for g in range(heads):
            kbuf[p, g] = kbuf[p, g].T
        return carry

    lax.fori_loop(0, pages, turn, 0, unroll=UNROLL)
    pltpu.make_async_copy(v_hbm, vbuf, vsem).wait()
    pltpu.make_async_copy(qall.at[pl.ds(0, n - 1)], qall.at[pl.ds(0, n - 1)], qr_sem).wait()

    row_group = (iota((32, width), 0) // 4) % 4
    low_half = iota((16, page_len), 0) % 8 < 4
    lanes = iota((16, page_len), 1)
    chunk = sbuf.shape[0]
    page_bits = pages.bit_length() - 1
    slot_bits = slots.bit_length() - 1

    def decode(k):
        code = meta_s[0, k]
        slot = jnp.bitwise_and(code >> page_bits, slots - 1)
        seq = jnp.bitwise_and(code >> (page_bits + slot_bits), seqs - 1)
        return jnp.bitwise_and(code, pages - 1), seq, slot

    def scores(k, pair):
        lhs, rhs = [], []
        for at in (k, k + 1):
            p, s, _ = decode(at)
            qb = qall[pl.ds(2 * s, 2)].reshape(32, width)
            none = jnp.zeros_like(qb)
            lhs.append(
                jnp.concatenate([jnp.where(row_group == 2 * pair + u, qb, none) for u in range(2)], axis=1)
            )
            rhs.append(kbuf[p, pl.ds(2 * pair, 2)].reshape(2 * width, page_len))
        raw = dot(jnp.concatenate(lhs, axis=0), jnp.concatenate(rhs, axis=1))
        a, b = 8 * pair, 16 + 8 * pair
        return (
            jnp.concatenate([raw[a : a + 8, :page_len], raw[b : b + 8, :page_len]], axis=0),
            jnp.concatenate([raw[32 + a : 40 + a, page_len:], raw[32 + b : 40 + b, page_len:]], axis=0),
        )

    def attend(k, pair, raw, state):
        m, l, acc = state
        p, s, slot = decode(k)
        before_seq = decode(jnp.maximum(k - 1, 0))[1]
        first = jnp.logical_or(k == 0, before_seq != s)
        valid = len_ref[s] - 1 - slot * page_len
        raw = jnp.where(lanes < valid, raw, LOW)
        top = jnp.maximum(jnp.max(raw, axis=1, keepdims=True), FLOOR)
        weights = jnp.exp2((raw - top) * c)
        total = jnp.sum(weights, axis=1, keepdims=True)
        lhs = jnp.concatenate(
            [jnp.where(low_half, weights, 0.0).astype(BF16), jnp.where(low_half, 0.0, weights).astype(BF16)], axis=1
        )
        page_out = dot(lhs, vbuf[p, pl.ds(2 * pair, 2)].reshape(2 * page_len, width))
        top = jnp.broadcast_to(top, m.shape)
        m = jnp.where(first, FLOOR, m)
        new_m = jnp.maximum(m, top)
        old = jnp.where(first, 0.0, jnp.exp2((m - new_m) * c))
        new = jnp.exp2((top - new_m) * c)
        l = l * old + total * new
        acc = acc * old + page_out * new
        racc[k] = acc
        rml[k] = jnp.where(lanes < 64, new_m, l)
        return new_m, l, acc

    zero = jnp.zeros((16, width), F32)
    steps = pages // chunk
    lane8 = iota((8, width), 1) % 64
    left = iota((n, width), 1) < 64
    for pair in range(2):

        ahead = 8
        raws = {}
        state = (zero, zero, zero)
        for k in range(0, ahead, 2):
            raws[k], raws[k + 1] = scores(k, pair)
        for k in range(0, pages, 2):
            if k + ahead < pages:
                raws[k + ahead], raws[k + ahead + 1] = scores(k + ahead, pair)
            for u in (k, k + 1):
                state = attend(u, pair, raws.pop(u), state)

        def gather(s, stat):
            end = meta_s[0, pages + s]
            start = jnp.where(s == 0, 0, meta_s[0, pages + jnp.maximum(s - 1, 0)])
            some = end > start
            last = jnp.clip(end - 1, 0, pages - 1)
            acc = jnp.where(some, racc[last], 0.0)
            ml = jnp.where(some, rml[last], jnp.where(lanes < 64, FLOOR, 0.0))
            mine[pair, 2 * s, 0:8] = acc[:8]
            mine[pair, 2 * s + 1, 0:8] = acc[8:]
            stat = jnp.where(lane8 == 2 * s, ml[:8], stat)
            return jnp.where(lane8 == 2 * s + 1, ml[8:], stat)

        stat = lax.fori_loop(0, seqs, gather, jnp.zeros((8, width), F32), unroll=4)
        turned = jnp.concatenate([stat] * 16, axis=0).T
        mine[pair, :, 8, :] = jnp.where(left, turned[:n], turned[n:])
        for t in order:
            pltpu.make_async_remote_copy(
                src_ref=mine.at[pair, jnp.bitwise_xor(me, t)], dst_ref=sent.at[pair, me],
                send_sem=out_sem.at[pair], recv_sem=in_sem.at[pair],
                device_id=peer(t), device_id_type=pl.DeviceIdType.MESH,
            ).start()
        sent[pair, me] = mine[pair, me]

    at_row = iota((8, width), 1) % 8 == iota((8, width), 0)
    first8 = jnp.logical_and(at_row, iota((8, width), 1) < 8)
    in_block = iota((16, width), 1) // 8 == iota((16, width), 0)
    for pair in range(2):
        some = sent.at[pair, pl.ds(0, n - 1)]
        pltpu.make_async_copy(some, some, in_sem.at[pair]).wait()
        stats = sent[pair, :, 8, :]
        turned = pltpu.roll(stats, 64, axis=1)
        tops = jnp.where(left, stats, turned)
        top = jnp.max(tops, axis=0, keepdims=True)
        w = jnp.exp2((tops - top) * c)
        total = jnp.sum(w * turned, axis=0, keepdims=True)
        top8 = jnp.sum(jnp.where(first8, top, 0.0), axis=1, keepdims=True)
        sum8 = jnp.sum(jnp.where(first8, total, 0.0), axis=1, keepdims=True)
        blocks = []
        for b in range(n // 16):
            line = jnp.sum(jnp.where(in_block, w[16 * b : 16 * b + 16], 0.0), axis=0, keepdims=True)
            blocks.append(jnp.where(at_row, line, 0.0))
        wide = jnp.concatenate(blocks, axis=1)
        wide_hi = wide.astype(BF16).astype(F32)
        lhs = jnp.concatenate([wide_hi, wide - wide_hi], axis=0).astype(BF16)
        parts = sent[pair, :, 0:8, :].reshape(8 * n, width)
        parts_hi = parts.astype(BF16)
        parts_lo = (parts - parts_hi.astype(F32)).astype(BF16)
        both = dot(lhs, parts_hi)
        numer = both[:8] + both[8:] + dot(lhs, parts_lo)[:8]
        rows = slice(8 * pair, 8 * pair + 8)
        high = jnp.maximum(top8, new_raw[rows])
        old = jnp.exp2((top8 - high) * c)
        new = jnp.exp2((new_raw[rows] - high) * c)
        result = (numer * old + new * vn16[rows]) / (sum8 * old + new)
        out_ref[rows] = result

    some = qall.at[pl.ds(0, n - 1)]
    pltpu.make_async_copy(some, some, qs_sem).wait()
    for pair in range(2):
        some = mine.at[pair, pl.ds(0, n - 1)]
        pltpu.make_async_copy(some, some, out_sem.at[pair]).wait()


def on_device(queries, key_cache, value_cache, key_new, value_new, lengths, page_table):
    n = lax.axis_size("kv")
    heads, rows, width = queries.shape
    pages, _, page_len, _ = key_cache.shape
    seqs = lengths.shape[0]
    vmem = pl.BlockSpec(memory_space=pltpu.VMEM)
    hbm = pl.BlockSpec(memory_space=pltpu.HBM)
    dma = pltpu.SemaphoreType.DMA
    inputs = (queries, key_cache, value_cache, key_new, value_new, lengths, page_table.reshape(seqs, -1))
    out = pl.pallas_call(
        functools.partial(kernel, n),
        out_shape=jax.ShapeDtypeStruct((heads * rows, width), F32),
        in_specs=[hbm] * 7,
        out_specs=vmem,
        scratch_shapes=[
            pltpu.VMEM(queries.shape, BF16),
            pltpu.VMEM((heads, width), BF16),
            pltpu.VMEM((heads, width), BF16),
            pltpu.SMEM((seqs,), jnp.int32),
            pltpu.VMEM((seqs, page_table.shape[0] // seqs), jnp.int32),
            pltpu.VMEM(key_cache.shape, BF16),
            pltpu.VMEM(value_cache.shape, BF16),
            pltpu.VMEM((n, 16, width), BF16),
            pltpu.VMEM((pages, 16, width), F32),
            pltpu.VMEM((pages, 16, width), F32),
            pltpu.VMEM((32, 16, page_len), F32),
            pltpu.VMEM((2, n, 9, width), F32),
            pltpu.VMEM((2, n, 9, width), F32),
            pltpu.VMEM((1, width), jnp.int32),
            pltpu.SMEM((1, width), jnp.int32),
            dma,
            dma,
            dma,
            dma((3,)),
            *[dma] * 4,
            dma((2,)),
            dma((2,)),
        ],
        compiler_params=pltpu.CompilerParams(
            collective_id=0, has_side_effects=True, vmem_limit_bytes=48 * 1024 * 1024
        ),
    )(*(pltpu.with_memory_space_constraint(x, pltpu.HBM) for x in inputs))
    return out.reshape(heads, rows, width).astype(BF16)


def solution(mesh):
    placed = (
        P("head", "kv", None),
        P("kv", "head", None, None),
        P("kv", "head", None, None),
        P(None, "head", None),
        P(None, "head", None),
        P(),
        P(),
    )
    return jax.shard_map(
        on_device, mesh=mesh, in_specs=placed, out_specs=P("head", "kv", None), check_vma=False
    )
```
